512 devices in a mesh: blk: 8 (over x, core), rows: 64 (over z, y).
Axes of the slice: x: 4, y: 8, z: 8, core: 2. Of those that a mesh axis runs over, the one named last changes fastest.
Arguments:
- snapshots: float32 [131072, 2048], P('rows', 'blk'), may hold values from -40 to 40
- grades: int32 [2048], P('blk'), may hold values from 0 to 7
- mover: int32 [3, 8], P(None, 'blk'), may hold values from 0 to 1
Outputs:
- basis: float32 [131072, 2048], P('rows', 'blk')
The draws below stay inside these ranges and needn't reach their ends.
All inputs are finite; a program needn't handle non-finite values.
Results may differ from the reference program's by a relative error of at most 0.0001.
Values sent between devices are 32-bit elements; how exact they have to be, the bound alone decides.
No kernel may reach another device: no remote copies, remote signals or barrier semaphores. Data moves between devices by JAX's collectives and lax.ppermute only.
A program may use at most 64 MiB of HBM per device.

```python
import math
import jax
import jax.numpy as jnp
from jax import lax

BW = 128
ROUNDS = 4
NS_STEPS = 3
GRADES = 8
ROWS = 131072
COLS = 2048
N_BLK = 8


factor_count = 32


def draw_snapshots(key, part):
    keys = jax.random.split(jax.random.fold_in(key, 11), 4)
    noise = jnp.clip(jax.random.normal(keys[0], (ROWS, COLS), jnp.float32), -6.0, 6.0)
    latent = jnp.clip(jax.random.normal(keys[1], (ROWS, factor_count), jnp.float32), -4.0, 4.0)
    decay = 0.04 * jnp.power(0.9, jnp.arange(factor_count, dtype=jnp.float32))
    loading = jax.random.uniform(keys[2], (factor_count, COLS), jnp.float32, -1.0, 1.0) * decay[:, None]
    common = jnp.dot(latent, loading, precision=jax.lax.Precision.HIGHEST)
    column_scale = jnp.exp(jax.random.uniform(keys[3], (1, COLS), jnp.float32, math.log(0.3), math.log(3.0)))
    values = (noise + common) * column_scale
    return jnp.clip(values, -40.0, 40.0)


def with_ends(entries, rng, least, top_value):
    extent = entries.shape
    index_at = [jax.random.randint(jax.random.fold_in(rng, axis), (), 0, extent[axis]) for axis in range(len(extent))]
    entries = entries.at[tuple(index_at)].set(least)
    longest = extent.index(max(extent))
    index_at[longest] = (index_at[longest] + 1) % extent[longest]
    return entries.at[tuple(index_at)].set(top_value)


def setup_inputs(seed: int = 0) -> dict:
    streams_of = jax.random.split(jax.random.key(seed), 4)
    return {
        "snapshots": draw_snapshots(jax.random.fold_in(streams_of[3], 71), 0),
        "grades": with_ends(jax.random.randint(streams_of[1], (COLS,), 0, GRADES), jax.random.fold_in(streams_of[1], 1), 0, GRADES - 1).astype(jnp.int32),
        "mover": with_ends(jax.random.randint(streams_of[2], (ROUNDS - 1, N_BLK), 0, 2), jax.random.fold_in(streams_of[2], 1), 0, 1).astype(jnp.int32),
    }


epsilon = 1e-06
relaxation = 1.2

def rotation(cross_gram, squares, labels):
    left_scale = lax.rsqrt(squares[:BW] + epsilon)
    right_scale = lax.rsqrt(squares[BW:] + epsilon)
    grade_gap = jnp.abs(labels[:BW, None] - labels[None, BW:])
    scaled = cross_gram * left_scale[:, None] * right_scale[None, :] / (1.0 + grade_gap)
    magnitude = jnp.sqrt(jnp.sum(scaled * scaled) + epsilon)
    generator = relaxation * scaled / magnitude
    zeros_block = jnp.zeros_like(generator)
    upper_half = jnp.concatenate([zeros_block, generator], 1)
    lower_half = jnp.concatenate([-generator.T, zeros_block], 1)
    iterate = jnp.eye(2 * BW, dtype=generator.dtype) + jnp.concatenate([upper_half, lower_half], 0)
    for sweep in range(NS_STEPS):
        product = lax.dot_general(iterate, iterate, (((0,), (0,)), ((), ())), precision=lax.Precision.HIGHEST)
        iterate = 1.5 * iterate - 0.5 * jnp.dot(iterate, product, precision=lax.Precision.HIGHEST)
    return iterate

def reference(snapshots, grades, mover):
    blocks = snapshots.reshape(ROWS, N_BLK, 2 * BW)
    labels = grades.reshape(N_BLK, 2 * BW).astype(snapshots.dtype)
    for round_index in range(ROUNDS):
        cross_gram = jnp.einsum('mpi,mpj->pij', blocks[:, :, :BW], blocks[:, :, BW:], precision=lax.Precision.HIGHEST)
        squares = lax.optimization_barrier(jnp.sum(blocks * blocks, axis=0))
        rotator = jax.vmap(rotation)(cross_gram, squares, labels)
        blocks = jnp.einsum('mpi,pij->mpj', blocks, rotator, precision=lax.Precision.HIGHEST)
        if round_index + 1 < ROUNDS:
            first = mover[round_index] == 0
            first_blocks = first[None, :, None]
            first_labels = first[:, None]
            moving = jnp.where(first_blocks, blocks[:, :, :BW], blocks[:, :, BW:])
            staying = jnp.where(first_blocks, blocks[:, :, BW:], blocks[:, :, :BW])
            move_label = jnp.where(first_labels, labels[:, :BW], labels[:, BW:])
            stay_label = jnp.where(first_labels, labels[:, BW:], labels[:, :BW])
            moving = jnp.roll(moving, 1, axis=1)
            move_label = jnp.roll(move_label, 1, axis=0)
            blocks = jnp.where(first_blocks, jnp.concatenate([moving, staying], 2), jnp.concatenate([staying, moving], 2))
            labels = jnp.where(first_labels, jnp.concatenate([move_label, stay_label], 1), jnp.concatenate([stay_label, move_label], 1))
    return blocks.reshape(ROWS, COLS)
```

```python
import jax
import jax.numpy as jnp
from jax import lax
from jax.sharding import PartitionSpec as P

BW = 128
ROUNDS = 4
NS_STEPS = 3

epsilon = 1e-06
relaxation = 1.2
EXACT = lax.Precision.HIGHEST
APPLY = lax.Precision.HIGH


def mm(a, b, precision=EXACT):
    return jnp.dot(a, b, precision=precision)


def mm_t(a, b):
    return lax.dot_general(a, b, (((0,), (0,)), ((), ())), precision=EXACT)


def product_halves(left, right):
    return jnp.concatenate([mm_t(left, right[:, :BW]), mm_t(left, right[:, BW:])], 0)


def row_total(value):
    peers = lax.axis_size("rows")
    parts = value.reshape(peers, -1, BW)
    arrived = lax.all_to_all(parts, "rows", split_axis=0, concat_axis=0, tiled=True)
    part = arrived.sum(axis=0)
    copies = jnp.broadcast_to(part, parts.shape)
    whole = lax.all_to_all(copies, "rows", split_axis=0, concat_axis=0, tiled=True)
    return whole.reshape(value.shape)


def to_next(value):
    peers = lax.axis_size("blk")
    return lax.ppermute(value, "blk", [(i, (i + 1) % peers) for i in range(peers)])


def rotation(cross, squares_a, squares_b, labels_a, labels_b, swapped):
    scale_a = lax.rsqrt(squares_a + epsilon)
    scale_b = lax.rsqrt(squares_b + epsilon)
    gap = jnp.abs(labels_a[:, None] - labels_b[None, :])
    scaled = cross * scale_a[:, None] * scale_b[None, :] / (1.0 + gap)
    magnitude = jnp.sqrt(jnp.sum(scaled * scaled) + epsilon)
    gen = relaxation * scaled / magnitude
    gen = jnp.where(swapped, -gen, gen)
    gen_t = gen.T
    eye = jnp.eye(BW, dtype=jnp.float32)
    factors = []
    for gram in (mm(gen, gen_t), mm(gen_t, gen)):
        metric = eye + gram
        factor = None
        for sweep in range(NS_STEPS):
            step = 1.5 * eye - 0.5 * metric
            factor = step if factor is None else mm(factor, step)
            if sweep + 1 < NS_STEPS:
                metric = mm(mm(metric, step), step)
        factors.append(factor)
    f_a, f_b = factors
    corner = mm(gen, f_b)
    return jnp.concatenate([f_a, -corner.T], 0), jnp.concatenate([corner, f_b], 0)


def diagonal(block):
    keep = jnp.eye(BW, dtype=bool)
    return jnp.sum(jnp.where(keep, block, 0.0), axis=0)


def form(halves, cols):
    return mm(halves[: 2 * BW], cols[:BW]) + mm(halves[2 * BW :], cols[BW:])


def squares_after(gram, cols):
    return jnp.maximum(jnp.sum(cols * form(gram, cols), axis=0), 0.0)


def body(snapshots, grades, mover):
    labels = grades.astype(jnp.float32)
    labels_a, labels_b = labels[:BW], labels[BW:]
    swapped = jnp.zeros((), bool)
    pair = snapshots
    prev = to_next(pair)
    for stage in range(ROUNDS // 2):
        early, late = 2 * stage, 2 * stage + 1
        product = product_halves(pair, pair)
        gram = row_total(product)
        product = product_halves(pair, prev)
        cross_gram = row_total(product)
        col_a, col_b = rotation(
            gram[2 * BW : 3 * BW],
            diagonal(gram[:BW]),
            diagonal(gram[3 * BW :]),
            labels_a,
            labels_b,
            swapped,
        )
        first = mover[early, 0] == 0
        a_moves = first != swapped
        move = jnp.where(a_moves, col_a, col_b)
        stay = jnp.where(a_moves, col_b, col_a)
        move_label = jnp.where(a_moves, labels_a, labels_b)
        labels_a = jnp.where(a_moves, labels_b, labels_a)
        swapped = first
        extra = jnp.stack([squares_after(gram, move), move_label])
        sent = to_next(jnp.concatenate([move, jnp.pad(extra, ((0, 6), (0, 0)))], 0))
        prev_move, squares_b, labels_b = sent[: 2 * BW], sent[2 * BW], sent[2 * BW + 1]
        squares_a = squares_after(gram, stay)
        came = mm(prev, prev_move, APPLY)
        if late + 1 < ROUNDS:
            passed = to_next(came)
            prev_stay = to_next(stay)
            prev = jnp.concatenate([mm(prev, prev_stay, APPLY), passed], 1)
        pair = jnp.concatenate([mm(pair, stay, APPLY), came], 1)
        cross = mm_t(stay, form(cross_gram, prev_move))
        col_a, col_b = rotation(cross, squares_a, squares_b, labels_a, labels_b, swapped)
        if late + 1 == ROUNDS:
            cols = jnp.where(
                swapped, jnp.concatenate([col_b, col_a], 1), jnp.concatenate([col_a, col_b], 1)
            )
            return mm(pair, cols, APPLY)
        first = mover[late, 0] == 0
        a_moves = first != swapped
        move = jnp.where(a_moves, col_a, col_b)
        stay = jnp.where(a_moves, col_b, col_a)
        move_label = jnp.where(a_moves, labels_a, labels_b)
        labels_a = jnp.where(a_moves, labels_b, labels_a)
        swapped = first
        sent = to_next(jnp.concatenate([move, jnp.broadcast_to(move_label, (8, BW))], 0))
        prev_move, labels_b = sent[: 2 * BW], sent[2 * BW]
        prev_stay = to_next(stay)
        came = mm(prev, prev_move, APPLY)
        passed = to_next(came)
        prev = jnp.concatenate([mm(prev, prev_stay, APPLY), passed], 1)
        pair = jnp.concatenate([mm(pair, stay, APPLY), came], 1)


def solution(mesh):
    placed = (P("rows", "blk"), P("blk"), P(None, "blk"))
    return jax.shard_map(
        body, mesh=mesh, in_specs=placed, out_specs=P("rows", "blk"), check_vma=False
    )
```

```python
import functools

import jax
import jax.numpy as jnp
from jax import lax
from jax.experimental import pallas as pl
from jax.experimental.pallas import tpu as pltpu
from jax.sharding import PartitionSpec as P

BW = 128
ROUNDS = 4
NS_STEPS = 3
ROW_TILE = 512
PARAMS = pltpu.CompilerParams(vmem_limit_bytes=16 * 2**20)

epsilon = 1e-06
relaxation = 1.2
EXACT = lax.Precision.HIGHEST
F32 = jnp.float32


def mm(a, b):
    return jnp.dot(a, b, precision=EXACT, preferred_element_type=F32)


def mm_t(a, b):
    dims = (((0,), (0,)), ((), ()))
    return lax.dot_general(a, b, dims, precision=EXACT, preferred_element_type=F32)


def in_two(value):
    high = value.astype(jnp.bfloat16)
    return high, (value - high.astype(F32)).astype(jnp.bfloat16)


def apply(left, right):
    left_high, left_low = in_two(left)
    right_high, right_low = in_two(right)
    dot = functools.partial(jnp.dot, preferred_element_type=F32)
    return dot(left_high, right_high) + (dot(left_high, right_low) + dot(left_low, right_high))


def add_product(left, right, out_ref):
    whole = mm_t(left, right)

    @pl.when(pl.program_id(0) == 0)
    def _():
        out_ref[...] = jnp.zeros_like(out_ref)

    out_ref[: 2 * BW, :] += whole[:, :BW]
    out_ref[2 * BW :, :] += whole[:, BW:]


def product_kernel(left_ref, right_ref, out_ref):
    add_product(left_ref[...], right_ref[...], out_ref)


def square_kernel(left_ref, out_ref):
    value = left_ref[...]
    add_product(value, value, out_ref)


def tiled(width=2 * BW):
    return pl.BlockSpec((ROW_TILE, width), lambda i: (i, 0))


def whole(rows):
    return pl.BlockSpec((rows, BW), lambda i: (0, 0))


def shape(rows, cols=BW):
    return jax.ShapeDtypeStruct((rows, cols), F32)


def product_halves(left, right=None):
    args = (left,) if right is None else (left, right)
    return pl.pallas_call(
        square_kernel if right is None else product_kernel,
        grid=(left.shape[0] // ROW_TILE,),
        in_specs=[tiled() for _ in args],
        out_specs=whole(4 * BW),
        out_shape=shape(4 * BW),
        compiler_params=PARAMS,
    )(*args)


def rotate_kernel(with_gram, pair_ref, prev_ref, stay_ref, sent_ref, out_ref, came_ref, gram_ref=None):
    came = apply(prev_ref[...], sent_ref[: 2 * BW, :])
    stays = apply(pair_ref[...], stay_ref[: 2 * BW, :])
    came_ref[...] = came
    out_ref[:, :BW] = stays
    out_ref[:, BW:] = came
    if with_gram:
        new = out_ref[...]
        add_product(new, new, gram_ref)


def rotate(pair, prev, stay, sent, with_gram):
    rows = pair.shape[0]
    return pl.pallas_call(
        functools.partial(rotate_kernel, with_gram),
        grid=(rows // ROW_TILE,),
        in_specs=[tiled(), tiled(), whole(stay.shape[0]), whole(sent.shape[0])],
        out_specs=[tiled(), tiled(BW)] + [whole(4 * BW)] * with_gram,
        out_shape=[shape(rows, 2 * BW), shape(rows)] + [shape(4 * BW)] * with_gram,
        compiler_params=PARAMS,
    )(pair, prev, stay, sent)


def join_kernel(prev_ref, cols_ref, passed_ref, out_ref):
    out_ref[:, :BW] = apply(prev_ref[...], cols_ref[: 2 * BW, :])
    out_ref[:, BW:] = passed_ref[...]


def join(prev, cols, passed):
    rows = prev.shape[0]
    return pl.pallas_call(
        join_kernel,
        grid=(rows // ROW_TILE,),
        in_specs=[tiled(), whole(cols.shape[0]), tiled(BW)],
        out_specs=tiled(),
        out_shape=shape(rows, 2 * BW),
        compiler_params=PARAMS,
    )(prev, cols, passed)


def last_kernel(pair_ref, left_ref, right_ref, out_ref):
    pair = pair_ref[...]
    cols = jnp.concatenate([left_ref[: 2 * BW, :], right_ref[: 2 * BW, :]], 1)
    out_ref[...] = apply(pair, cols)


def last(pair, left, right):
    rows = pair.shape[0]
    return pl.pallas_call(
        last_kernel,
        grid=(rows // ROW_TILE,),
        in_specs=[tiled(), whole(left.shape[0]), whole(right.shape[0])],
        out_specs=tiled(),
        out_shape=shape(rows, 2 * BW),
        compiler_params=PARAMS,
    )(pair, left, right)


def form(halves, cols):
    return mm(halves[: 2 * BW], cols[:BW]) + mm(halves[2 * BW :], cols[BW:])


def columns_kernel(late, *refs):
    row_of = lax.broadcasted_iota(jnp.int32, (BW, BW), 0)
    keep = row_of == lax.broadcasted_iota(jnp.int32, (BW, BW), 1)
    eye = jnp.where(keep, 1.0, 0.0).astype(F32)

    def upright(row):
        return jnp.sum(jnp.where(keep, row, 0.0), axis=1, keepdims=True)

    if late:
        gram_ref, stay_ref, sent_ref, rows_ref, move_out, stay_out = refs
        gram = gram_ref[...]
        cross = mm_t(stay_ref[: 2 * BW, :], form(gram, sent_ref[: 2 * BW, :]))
        squares_a = stay_ref[2 * BW : 2 * BW + 1, :]
        squares_b = sent_ref[2 * BW : 2 * BW + 1, :]
    else:
        gram_ref, rows_ref, move_out, stay_out = refs
        gram = gram_ref[...]
        cross = gram[2 * BW : 3 * BW]
        squares_a = jnp.sum(jnp.where(keep, gram[:BW], 0.0), axis=0, keepdims=True)
        squares_b = jnp.sum(jnp.where(keep, gram[3 * BW :], 0.0), axis=0, keepdims=True)
    labels_a, labels_b = rows_ref[0:1, :], rows_ref[1:2, :]
    sign, a_moves = rows_ref[2:3, :], rows_ref[3:4, :] > 0.5
    scale_a = upright(lax.rsqrt(squares_a + epsilon))
    scale_b = lax.rsqrt(squares_b + epsilon)
    gap = jnp.abs(upright(labels_a) - labels_b)
    scaled = cross * scale_a * scale_b / (1.0 + gap)
    total = jnp.sum(jnp.sum(scaled * scaled, axis=0, keepdims=True), axis=1, keepdims=True)
    gen = relaxation * scaled / jnp.sqrt(total + epsilon) * sign
    gen_t = gen.T
    factors = []
    corner = gen
    metrics = [eye + mm(gen, gen_t), eye + mm(gen_t, gen)]
    for sweep in range(NS_STEPS):
        steps = [1.5 * eye - 0.5 * metric for metric in metrics]
        factors = [mm(f, s) for f, s in zip(factors, steps)] if factors else steps
        corner = mm(corner, steps[1])
        if sweep + 1 < NS_STEPS:
            metrics = [mm(mm(m, s), s) for m, s in zip(metrics, steps)]
    corner_t = -corner.T
    row = lax.broadcasted_iota(jnp.int32, (8, BW), 0)
    for out_ref, pick in ((move_out, a_moves), (stay_out, jnp.logical_not(a_moves))):
        top = jnp.where(pick, factors[0], corner)
        bottom = jnp.where(pick, corner_t, factors[1])
        out_ref[:BW, :] = top
        out_ref[BW : 2 * BW, :] = bottom
        tail = jnp.where(row == 1, jnp.where(pick, labels_a, labels_b), 0.0)
        if not late:
            image = form(gram, jnp.concatenate([top, bottom], 0))
            squares = jnp.sum(top * image[:BW], axis=0, keepdims=True)
            squares += jnp.sum(bottom * image[BW:], axis=0, keepdims=True)
            tail = jnp.where(row == 0, jnp.maximum(squares, 0.0), tail)
        out_ref[2 * BW :, :] = tail


def columns(args, labels_a, labels_b, swapped, a_moves):
    sign = jnp.where(swapped, -1.0, 1.0)
    pick = jnp.where(a_moves, 1.0, 0.0)
    row = lax.broadcasted_iota(jnp.int32, (8, BW), 0)
    rows = jnp.where(row == 2, sign, pick)
    rows = jnp.where(row == 0, labels_a, jnp.where(row == 1, labels_b, rows))
    return pl.pallas_call(
        functools.partial(columns_kernel, len(args) > 1),
        out_shape=[shape(2 * BW + 8)] * 2,
        compiler_params=PARAMS,
    )(*args, rows)


def exchange_all(parts):
    return lax.all_to_all(parts, "rows", split_axis=0, concat_axis=0, tiled=True)


def to_next(value):
    peers = lax.axis_size("blk")
    return lax.ppermute(value, "blk", [(i, (i + 1) % peers) for i in range(peers)])


def body(snapshots, grades, mover):
    peers = lax.axis_size("rows")
    labels = grades.astype(F32)
    labels_a, labels_b = labels[None, :BW], labels[None, BW:]
    swapped = jnp.zeros((), bool)
    pair = snapshots
    prev = to_next(pair)
    product = product_halves(pair)
    for stage in range(ROUNDS // 2):
        early, late = 2 * stage, 2 * stage + 1
        part = exchange_all(product.reshape(peers, -1, BW)).sum(axis=0)
        product = product_halves(pair, prev)
        lines = product.reshape(peers, -1, BW)
        copies = jnp.broadcast_to(part, lines.shape)
        both = exchange_all(jnp.concatenate([copies, lines], 1))
        gram = both[:, : lines.shape[1]].reshape(product.shape)
        part = both[:, lines.shape[1] :].sum(axis=0)
        cross_gram = exchange_all(jnp.broadcast_to(part, lines.shape)).reshape(product.shape)
        first = mover[early, 0] == 0
        a_moves = first != swapped
        move, stay = columns((gram,), labels_a, labels_b, swapped, a_moves)
        labels_a = stay[2 * BW + 1 : 2 * BW + 2]
        swapped = first
        sent = to_next(move)
        labels_b = sent[2 * BW + 1 : 2 * BW + 2]
        pair_next, came = rotate(pair, prev, stay, sent, False)
        if late + 1 < ROUNDS:
            passed = to_next(came)
            prev_stay = to_next(stay)
            prev = join(prev, prev_stay, passed)
        pair = pair_next
        if late + 1 == ROUNDS:
            a_moves = jnp.logical_not(swapped)
        else:
            first = mover[late, 0] == 0
            a_moves = first != swapped
        move, stay = columns((cross_gram, stay, sent), labels_a, labels_b, swapped, a_moves)
        if late + 1 == ROUNDS:
            return last(pair, move, stay)
        labels_a = stay[2 * BW + 1 : 2 * BW + 2]
        swapped = first
        sent = to_next(move)
        labels_b = sent[2 * BW + 1 : 2 * BW + 2]
        prev_stay = to_next(stay)
        pair, came, product = rotate(pair, prev, stay, sent, True)
        passed = to_next(came)
        prev = join(prev, prev_stay, passed)


def solution(mesh):
    placed = (P("rows", "blk"), P("blk"), P(None, "blk"))
    return jax.shard_map(
        body, mesh=mesh, in_specs=placed, out_specs=P("rows", "blk"), check_vma=False
    )
```

```python
import functools

import jax
import jax.numpy as jnp
from jax import lax
from jax.experimental import pallas as pl
from jax.experimental.pallas import tpu as pltpu
from jax.sharding import PartitionSpec as P

BW = 128
ROUNDS = 4
NS_STEPS = 3
ROW_TILE = 1024
PARAMS = pltpu.CompilerParams(vmem_limit_bytes=16 * 2**20)

epsilon = 1e-06
relaxation = 1.2
EXACT = lax.Precision.HIGHEST
F32 = jnp.float32


def mm(a, b):
    return jnp.dot(a, b, precision=EXACT, preferred_element_type=F32)


def mm_t(a, b):
    dims = (((0,), (0,)), ((), ()))
    return lax.dot_general(a, b, dims, precision=EXACT, preferred_element_type=F32)


def in_two(value):
    high = value.astype(jnp.bfloat16)
    return high, (value - high.astype(F32)).astype(jnp.bfloat16)


def apply(left, right):
    left_high, left_low = in_two(left)
    right_high, right_low = in_two(right)
    dot = functools.partial(jnp.dot, preferred_element_type=F32)
    return dot(left_high, right_high) + (dot(left_high, right_low) + dot(left_low, right_high))


def add_product(left, right, out_ref):
    dims = (((0,), (0,)), ((), ()))
    dot_t = functools.partial(lax.dot_general, dimension_numbers=dims, preferred_element_type=F32)
    left_high, left_low = in_two(left)
    if right is None:
        side = dot_t(left_high, left_low)
        whole = dot_t(left_high, left_high) + (side + side.T)
    else:
        right_high, right_low = in_two(right)
        cross = dot_t(left_high, right_low) + dot_t(left_low, right_high)
        whole = dot_t(left_high, right_high) + cross

    @pl.when(pl.program_id(0) == 0)
    def _():
        out_ref[...] = jnp.zeros_like(out_ref)

    out_ref[: 2 * BW, :] += whole[:, :BW]
    out_ref[2 * BW :, :] += whole[:, BW:]


def product_kernel(left_ref, right_ref, out_ref):
    add_product(left_ref[...], right_ref[...], out_ref)


def square_kernel(left_ref, out_ref):
    add_product(left_ref[...], None, out_ref)


def tiled(width=2 * BW):
    return pl.BlockSpec((ROW_TILE, width), lambda i: (i, 0))


def whole(rows):
    return pl.BlockSpec((rows, BW), lambda i: (0, 0))


def shape(rows, cols=BW):
    return jax.ShapeDtypeStruct((rows, cols), F32)


def streamed(value):
    return pltpu.with_memory_space_constraint(value, pltpu.HBM)


def product_halves(left, right=None):
    left = streamed(left)
    args = (left,) if right is None else (left, right)
    return pl.pallas_call(
        square_kernel if right is None else product_kernel,
        grid=(left.shape[0] // ROW_TILE,),
        in_specs=[tiled() for _ in args],
        out_specs=whole(4 * BW),
        out_shape=shape(4 * BW),
        compiler_params=PARAMS,
    )(*args)


def rotate_kernel(pair_ref, prev_ref, stay_ref, sent_ref, out_ref, came_ref=None, gram_ref=None):
    came = apply(prev_ref[...], sent_ref[: 2 * BW, :])
    stays = apply(pair_ref[...], stay_ref[: 2 * BW, :])
    out_ref[:, :BW] = stays
    out_ref[:, BW:] = came
    if gram_ref is not None:
        came_ref[...] = came
        add_product(jnp.concatenate([stays, came], 1), None, gram_ref)


def rotate(pair, prev, stay, sent, with_gram=False):
    rows = pair.shape[0]
    pair = streamed(pair)
    if with_gram:
        prev = streamed(prev)
    out_specs = (tiled(), tiled(BW), whole(4 * BW))
    out_shape = (pltpu.HBM((rows, 2 * BW), F32), shape(rows), shape(4 * BW))
    return pl.pallas_call(
        rotate_kernel,
        grid=(rows // ROW_TILE,),
        in_specs=[tiled(), tiled(), whole(stay.shape[0]), whole(sent.shape[0])],
        out_specs=out_specs if with_gram else out_specs[0],
        out_shape=out_shape if with_gram else out_shape[0],
        compiler_params=PARAMS,
    )(pair, prev, stay, sent)


def join_kernel(prev_ref, cols_ref, passed_ref, out_ref):
    out_ref[:, :BW] = apply(prev_ref[...], cols_ref[: 2 * BW, :])
    out_ref[:, BW:] = passed_ref[...]


def join_two_kernel(prev_ref, cols_ref, other_ref, other_cols_ref, out_ref):
    out_ref[:, :BW] = apply(prev_ref[...], cols_ref[: 2 * BW, :])
    out_ref[:, BW:] = apply(other_ref[...], other_cols_ref[: 2 * BW, :])


def join(prev, cols, passed, passed_cols=None):
    rows = prev.shape[0]
    if passed_cols is None:
        prev = streamed(prev)
    args = (prev, cols, passed) if passed_cols is None else (prev, cols, passed, passed_cols)
    return pl.pallas_call(
        join_kernel if passed_cols is None else join_two_kernel,
        grid=(rows // ROW_TILE,),
        in_specs=[tiled(a.shape[1]) if a.shape[0] == rows else whole(a.shape[0]) for a in args],
        out_specs=tiled(),
        out_shape=shape(rows, 2 * BW) if passed_cols is None else pltpu.HBM((rows, 2 * BW), F32),
        compiler_params=PARAMS,
    )(*args)


def last_kernel(pair_ref, left_ref, right_ref, out_ref):
    pair = pair_ref[...]
    cols = jnp.concatenate([left_ref[: 2 * BW, :], right_ref[: 2 * BW, :]], 1)
    out_ref[...] = apply(pair, cols)


def last(pair, left, right):
    pair = streamed(pair)
    rows = pair.shape[0]
    return pl.pallas_call(
        last_kernel,
        grid=(rows // ROW_TILE,),
        in_specs=[tiled(), whole(left.shape[0]), whole(right.shape[0])],
        out_specs=tiled(),
        out_shape=shape(rows, 2 * BW),
        compiler_params=PARAMS,
    )(pair, left, right)


def form(halves, cols):
    return mm(halves[: 2 * BW], cols[:BW]) + mm(halves[2 * BW :], cols[BW:])


def columns_kernel(late, *refs):
    row_of = lax.broadcasted_iota(jnp.int32, (BW, BW), 0)
    keep = row_of == lax.broadcasted_iota(jnp.int32, (BW, BW), 1)
    eye = jnp.where(keep, 1.0, 0.0).astype(F32)

    def upright(row):
        return jnp.sum(jnp.where(keep, row, 0.0), axis=1, keepdims=True)

    if late:
        gram_ref, stay_ref, sent_ref, rows_ref, move_out, stay_out = refs
        gram = gram_ref[...]
        cross = mm_t(stay_ref[: 2 * BW, :], form(gram, sent_ref[: 2 * BW, :]))
        squares_a = stay_ref[2 * BW : 2 * BW + 1, :]
        squares_b = sent_ref[2 * BW : 2 * BW + 1, :]
    else:
        gram_ref, rows_ref, move_out, stay_out = refs
        gram = gram_ref[...]
        cross = gram[2 * BW : 3 * BW]
        squares_a = jnp.sum(jnp.where(keep, gram[:BW], 0.0), axis=0, keepdims=True)
        squares_b = jnp.sum(jnp.where(keep, gram[3 * BW :], 0.0), axis=0, keepdims=True)
    labels_a, labels_b = rows_ref[0:1, :], rows_ref[1:2, :]
    sign, a_moves = rows_ref[2:3, :], rows_ref[3:4, :] > 0.5
    scale_a = upright(lax.rsqrt(squares_a + epsilon))
    scale_b = lax.rsqrt(squares_b + epsilon)
    gap = jnp.abs(upright(labels_a) - labels_b)
    scaled = cross * scale_a * scale_b / (1.0 + gap)
    total = jnp.sum(jnp.sum(scaled * scaled, axis=0, keepdims=True), axis=1, keepdims=True)
    gen = relaxation * scaled / jnp.sqrt(total + epsilon) * sign
    gen_t = gen.T
    factors = []
    corner = gen
    metrics = [eye + mm(gen, gen_t), eye + mm(gen_t, gen)]
    for sweep in range(NS_STEPS):
        steps = [1.5 * eye - 0.5 * metric for metric in metrics]
        factors = [mm(f, s) for f, s in zip(factors, steps)] if factors else steps
        corner = mm(corner, steps[1])
        if sweep + 1 < NS_STEPS:
            metrics = [mm(mm(m, s), s) for m, s in zip(metrics, steps)]
    corner_t = -corner.T
    row = lax.broadcasted_iota(jnp.int32, (8, BW), 0)
    for out_ref, pick in ((move_out, a_moves), (stay_out, jnp.logical_not(a_moves))):
        top = jnp.where(pick, factors[0], corner)
        bottom = jnp.where(pick, corner_t, factors[1])
        out_ref[:BW, :] = top
        out_ref[BW : 2 * BW, :] = bottom
        tail = jnp.where(row == 1, jnp.where(pick, labels_a, labels_b), 0.0)
        if not late:
            image = form(gram, jnp.concatenate([top, bottom], 0))
            squares = jnp.sum(top * image[:BW], axis=0, keepdims=True)
            squares += jnp.sum(bottom * image[BW:], axis=0, keepdims=True)
            tail = jnp.where(row == 0, jnp.maximum(squares, 0.0), tail)
        out_ref[2 * BW :, :] = tail


def columns(args, labels_a, labels_b, swapped, a_moves):
    sign = jnp.where(swapped, -1.0, 1.0)
    pick = jnp.where(a_moves, 1.0, 0.0)
    row = lax.broadcasted_iota(jnp.int32, (8, BW), 0)
    rows = jnp.where(row == 2, sign, pick)
    rows = jnp.where(row == 0, labels_a, jnp.where(row == 1, labels_b, rows))
    return pl.pallas_call(
        functools.partial(columns_kernel, len(args) > 1),
        out_shape=[shape(2 * BW + 8)] * 2,
        compiler_params=PARAMS,
    )(*args, rows)


def exchange_all(parts):
    flat = parts.reshape(parts.shape[0], 1, -1)
    return lax.all_to_all(flat, "rows", split_axis=0, concat_axis=0, tiled=True).reshape(parts.shape)


def to_next(value):
    peers = lax.axis_size("blk")
    return lax.ppermute(value, "blk", [(i, (i + 1) % peers) for i in range(peers)])


def body(snapshots, grades, mover):
    peers = lax.axis_size("rows")
    labels = grades.astype(F32)
    labels_a, labels_b = labels[None, :BW], labels[None, BW:]
    swapped = jnp.zeros((), bool)
    pair = snapshots
    prev = to_next(pair)
    product = product_halves(pair)
    for stage in range(ROUNDS // 2):
        early, late = 2 * stage, 2 * stage + 1
        part = exchange_all(product.reshape(peers, -1, BW)).sum(axis=0)
        product = product_halves(pair, prev)
        lines = product.reshape(peers, -1, BW)
        copies = jnp.broadcast_to(part, lines.shape)
        if late + 1 < ROUNDS:
            before = to_next(prev)
        both = exchange_all(jnp.concatenate([copies, lines], 1))
        gram = both[:, : lines.shape[1]].reshape(product.shape)
        part = both[:, lines.shape[1] :].sum(axis=0)
        cross_gram = exchange_all(jnp.broadcast_to(part, lines.shape)).reshape(product.shape)
        first = mover[early, 0] == 0
        a_moves = first != swapped
        move, stay = columns((gram,), labels_a, labels_b, swapped, a_moves)
        labels_a = stay[2 * BW + 1 : 2 * BW + 2]
        swapped = first
        sent = to_next(move)
        labels_b = sent[2 * BW + 1 : 2 * BW + 2]
        pair = rotate(pair, prev, stay, sent)
        if late + 1 < ROUNDS:
            prev_stay = to_next(stay)
            sent_before = to_next(sent)
            prev = join(prev, prev_stay, before, sent_before)
        if late + 1 == ROUNDS:
            a_moves = jnp.logical_not(swapped)
        else:
            first = mover[late, 0] == 0
            a_moves = first != swapped
        move, stay = columns((cross_gram, stay, sent), labels_a, labels_b, swapped, a_moves)
        if late + 1 == ROUNDS:
            return last(pair, move, stay)
        labels_a = stay[2 * BW + 1 : 2 * BW + 2]
        swapped = first
        sent = to_next(move)
        labels_b = sent[2 * BW + 1 : 2 * BW + 2]
        prev_stay = to_next(stay)
        pair, came, product = rotate(pair, prev, stay, sent, True)
        passed = to_next(came)
        prev = join(prev, prev_stay, passed)


def solution(mesh):
    placed = (P("rows", "blk"), P("blk"), P(None, "blk"))
    return jax.shard_map(
        body, mesh=mesh, in_specs=placed, out_specs=P("rows", "blk"), check_vma=False
    )
```

```python
import functools

import jax
import jax.numpy as jnp
from jax import lax
from jax.experimental import pallas as pl
from jax.experimental.pallas import tpu as pltpu
from jax.sharding import PartitionSpec as P

BW = 128
ROUNDS = 4
NS_STEPS = 3
ROW_TILE = 1024
PACKED = 5 * 64
PARAMS = pltpu.CompilerParams(vmem_limit_bytes=16 * 2**20)

epsilon = 1e-06
relaxation = 1.2
EXACT = lax.Precision.HIGHEST
F32 = jnp.float32


def mm(a, b):
    return jnp.dot(a, b, precision=EXACT, preferred_element_type=F32)


def mm_t(a, b):
    dims = (((0,), (0,)), ((), ()))
    return lax.dot_general(a, b, dims, precision=EXACT, preferred_element_type=F32)


def in_two(value):
    high = value.astype(jnp.bfloat16)
    return high, (value - high.astype(F32)).astype(jnp.bfloat16)


def apply(left, right):
    left_high, left_low = in_two(left)
    right_high, right_low = in_two(right)
    dot = functools.partial(jnp.dot, preferred_element_type=F32)
    return dot(left_high, right_high) + (dot(left_high, right_low) + dot(left_low, right_high))


def transposed_dot(left, right):
    dims = (((0,), (0,)), ((), ()))
    return lax.dot_general(left, right, dims, preferred_element_type=F32)


def unit():
    row = lax.broadcasted_iota(jnp.int32, (BW, BW), 0)
    return row, lax.broadcasted_iota(jnp.int32, (BW, BW), 1)


def product_kernel(left_ref, right_ref, out_ref):
    left_high, left_low = in_two(left_ref[...])
    right_high, right_low = in_two(right_ref[...])
    cross = transposed_dot(left_high, right_low) + transposed_dot(left_low, right_high)
    value = transposed_dot(left_high, right_high) + cross

    @pl.when(pl.program_id(0) == 0)
    def _():
        out_ref[...] = jnp.zeros_like(out_ref)

    out_ref[: 2 * BW, :] += value[:, :BW]
    out_ref[2 * BW :, :] += value[:, BW:]


def add_square(value, total_ref, out_ref):
    high, low = in_two(value)
    side = transposed_dot(high, low)
    value = transposed_dot(high, high) + (side + side.T)
    step = pl.program_id(0)

    @pl.when(step == 0)
    def _():
        total_ref[...] = value

    @pl.when(step > 0)
    def _():
        total_ref[...] += value

    @pl.when(step == pl.num_programs(0) - 1)
    def _():
        row, col = unit()
        second = total_ref[BW:, BW:]
        out_ref[:BW, :] = total_ref[:BW, BW:]
        out_ref[BW : 2 * BW, :] = jnp.where(row <= col, total_ref[:BW, :BW], second)
        ends = jnp.sum(jnp.where(row == col, second, 0.0), axis=0, keepdims=True)
        out_ref[2 * BW :, :] = jnp.broadcast_to(ends, (PACKED - 2 * BW, BW))


def unpacked(packed):
    row, col = unit()
    mixed = packed[BW : 2 * BW]
    turned = mixed.T
    ends = packed[2 * BW : 2 * BW + 1]
    first = jnp.where(row <= col, mixed, turned)
    second = jnp.where(row > col, mixed, jnp.where(row < col, turned, ends))
    return packed[:BW], first, second


def square_kernel(value_ref, out_ref, total_ref):
    add_square(value_ref[...], total_ref, out_ref)


TOTAL = pltpu.VMEM((2 * BW, 2 * BW), F32)


def tiled(width=2 * BW):
    return pl.BlockSpec((ROW_TILE, width), lambda i: (i, 0))


def whole(rows):
    return pl.BlockSpec((rows, BW), lambda i: (0, 0))


def shape(rows, cols=BW):
    return jax.ShapeDtypeStruct((rows, cols), F32)


def streamed(value):
    return pltpu.with_memory_space_constraint(value, pltpu.HBM)


def square(value):
    return pl.pallas_call(
        square_kernel,
        grid=(value.shape[0] // ROW_TILE,),
        in_specs=[tiled()],
        out_specs=whole(PACKED),
        out_shape=shape(PACKED),
        scratch_shapes=[TOTAL],
        compiler_params=PARAMS,
    )(streamed(value))


def product_halves(left, right):
    return pl.pallas_call(
        product_kernel,
        grid=(left.shape[0] // ROW_TILE,),
        in_specs=[tiled(), tiled()],
        out_specs=whole(4 * BW),
        out_shape=shape(4 * BW),
        compiler_params=PARAMS,
    )(streamed(left), right)


def share_kernel(peers, arrived_ref, lines_ref, out_ref):
    packed, lines = PACKED // peers, 4 * BW // peers
    part = arrived_ref[:packed, :]
    for i in range(1, peers):
        part += arrived_ref[packed * i : packed * (i + 1), :]
    for i in range(peers):
        at = (packed + lines) * i
        out_ref[at : at + packed, :] = part
        out_ref[at + packed : at + packed + lines, :] = lines_ref[lines * i : lines * (i + 1), :]


def split_kernel(peers, both_ref, packed_ref, out_ref):
    packed, lines = PACKED // peers, 4 * BW // peers
    part = both_ref[packed : packed + lines, :]
    for i in range(1, peers):
        at = (packed + lines) * i + packed
        part += both_ref[at : at + lines, :]
    for i in range(peers):
        out_ref[lines * i : lines * (i + 1), :] = part
    for i in range(peers):
        at = (packed + lines) * i
        packed_ref[packed * i : packed * (i + 1), :] = both_ref[at : at + packed, :]


def rotate_kernel(pair_ref, prev_ref, stay_ref, sent_ref, out_ref, came_ref=None, gram_ref=None, total_ref=None):
    came = apply(prev_ref[...], sent_ref[: 2 * BW, :])
    stays = apply(pair_ref[...], stay_ref[: 2 * BW, :])
    out_ref[:, :BW] = stays
    out_ref[:, BW:] = came
    if gram_ref is not None:
        came_ref[...] = came
        add_square(jnp.concatenate([stays, came], 1), total_ref, gram_ref)


def rotate(pair, prev, stay, sent, with_gram=False):
    rows = pair.shape[0]
    if with_gram:
        prev = streamed(prev)
    else:
        pair = streamed(pair)
    out_specs = (tiled(), tiled(BW), whole(PACKED))
    out_shape = (pltpu.HBM((rows, 2 * BW), F32), shape(rows), shape(PACKED))
    return pl.pallas_call(
        rotate_kernel,
        grid=(rows // ROW_TILE,),
        in_specs=[tiled(), tiled(), whole(stay.shape[0]), whole(sent.shape[0])],
        out_specs=out_specs if with_gram else out_specs[0],
        out_shape=out_shape if with_gram else out_shape[0],
        scratch_shapes=[TOTAL] if with_gram else [],
        compiler_params=PARAMS,
    )(pair, prev, stay, sent)


def join_kernel(prev_ref, cols_ref, passed_ref, out_ref):
    out_ref[:, :BW] = apply(prev_ref[...], cols_ref[: 2 * BW, :])
    out_ref[:, BW:] = passed_ref[...]


def join_two_kernel(prev_ref, cols_ref, other_ref, other_cols_ref, out_ref):
    out_ref[:, :BW] = apply(prev_ref[...], cols_ref[: 2 * BW, :])
    out_ref[:, BW:] = apply(other_ref[...], other_cols_ref[: 2 * BW, :])


def join(prev, cols, passed, passed_cols=None):
    rows = prev.shape[0]
    if passed_cols is None:
        prev = streamed(prev)
    args = (prev, cols, passed) if passed_cols is None else (prev, cols, passed, passed_cols)
    return pl.pallas_call(
        join_kernel if passed_cols is None else join_two_kernel,
        grid=(rows // ROW_TILE,),
        in_specs=[tiled(a.shape[1]) if a.shape[0] == rows else whole(a.shape[0]) for a in args],
        out_specs=tiled(),
        out_shape=shape(rows, 2 * BW) if passed_cols is None else pltpu.HBM((rows, 2 * BW), F32),
        compiler_params=PARAMS,
    )(*args)


def last_kernel(pair_ref, left_ref, right_ref, out_ref):
    pair = pair_ref[...]
    cols = jnp.concatenate([left_ref[: 2 * BW, :], right_ref[: 2 * BW, :]], 1)
    out_ref[...] = apply(pair, cols)


def last(pair, left, right):
    pair = streamed(pair)
    rows = pair.shape[0]
    return pl.pallas_call(
        last_kernel,
        grid=(rows // ROW_TILE,),
        in_specs=[tiled(), whole(left.shape[0]), whole(right.shape[0])],
        out_specs=tiled(),
        out_shape=shape(rows, 2 * BW),
        compiler_params=PARAMS,
    )(pair, left, right)


def form(halves, cols):
    return mm(halves[: 2 * BW], cols[:BW]) + mm(halves[2 * BW :], cols[BW:])


def columns_kernel(late, *refs):
    row_of, col_of = unit()
    keep = row_of == col_of
    eye = jnp.where(keep, 1.0, 0.0).astype(F32)

    def upright(row):
        return jnp.sum(jnp.where(keep, row, 0.0), axis=1, keepdims=True)

    if late:
        gram_ref, stay_ref, sent_ref, rows_ref, move_out, stay_out = refs
        gram = gram_ref[...]
        cross = mm_t(stay_ref[: 2 * BW, :], form(gram, sent_ref[: 2 * BW, :]))
        squares_a = stay_ref[2 * BW : 2 * BW + 1, :]
        squares_b = sent_ref[2 * BW : 2 * BW + 1, :]
    else:
        gram_ref, rows_ref, move_out, stay_out = refs
        cross, within_a, within_b = unpacked(gram_ref[...])
        squares_a = jnp.sum(jnp.where(keep, within_a, 0.0), axis=0, keepdims=True)
        squares_b = gram_ref[2 * BW : 2 * BW + 1, :]
        cross_t = cross.T
    labels_a, labels_b = rows_ref[0:1, :], rows_ref[1:2, :]
    sign, a_moves = rows_ref[2:3, :], rows_ref[3:4, :] > 0.5
    scale_a = upright(lax.rsqrt(squares_a + epsilon))
    scale_b = lax.rsqrt(squares_b + epsilon)
    gap = jnp.abs(upright(labels_a) - labels_b)
    scaled = cross * scale_a * scale_b / (1.0 + gap)
    total = jnp.sum(jnp.sum(scaled * scaled, axis=0, keepdims=True), axis=1, keepdims=True)
    gen = relaxation * scaled / jnp.sqrt(total + epsilon) * sign
    gen_t = gen.T
    factors = []
    corner = gen
    metrics = [eye + mm(gen, gen_t), eye + mm(gen_t, gen)]
    for sweep in range(NS_STEPS):
        steps = [1.5 * eye - 0.5 * metric for metric in metrics]
        factors = [mm(f, s) for f, s in zip(factors, steps)] if factors else steps
        corner = mm(corner, steps[1])
        if sweep + 1 < NS_STEPS:
            metrics = [mm(mm(m, s), s) for m, s in zip(metrics, steps)]
    corner_t = -corner.T
    row = lax.broadcasted_iota(jnp.int32, (8, BW), 0)
    for out_ref, pick in ((move_out, a_moves), (stay_out, jnp.logical_not(a_moves))):
        top = jnp.where(pick, factors[0], corner)
        bottom = jnp.where(pick, corner_t, factors[1])
        out_ref[:BW, :] = top
        out_ref[BW : 2 * BW, :] = bottom
        tail = jnp.where(row == 1, jnp.where(pick, labels_a, labels_b), 0.0)
        if not late:
            image_a = mm(within_a, top) + mm(cross, bottom)
            image_b = mm(cross_t, top) + mm(within_b, bottom)
            squares = jnp.sum(top * image_a + bottom * image_b, axis=0, keepdims=True)
            tail = jnp.where(row == 0, jnp.maximum(squares, 0.0), tail)
        out_ref[2 * BW :, :] = tail


def columns(args, labels_a, labels_b, swapped, a_moves):
    sign = jnp.where(swapped, -1.0, 1.0)
    pick = jnp.where(a_moves, 1.0, 0.0)
    row = lax.broadcasted_iota(jnp.int32, (8, BW), 0)
    rows = jnp.where(row == 2, sign, pick)
    rows = jnp.where(row == 0, labels_a, jnp.where(row == 1, labels_b, rows))
    return pl.pallas_call(
        functools.partial(columns_kernel, len(args) > 1),
        out_shape=[shape(2 * BW + 8)] * 2,
        compiler_params=PARAMS,
    )(*args, rows)


def exchange_all(parts):
    flat = parts.reshape(lax.axis_size("rows"), 1, -1)
    return lax.all_to_all(flat, "rows", split_axis=0, concat_axis=0, tiled=True).reshape(parts.shape)


def to_next(value):
    peers = lax.axis_size("blk")
    return lax.ppermute(value, "blk", [(i, (i + 1) % peers) for i in range(peers)])


def body(snapshots, grades, mover):
    peers = lax.axis_size("rows")
    labels = grades.astype(F32)
    labels_a, labels_b = labels[None, :BW], labels[None, BW:]
    swapped = jnp.zeros((), bool)
    pair = snapshots
    prev = to_next(pair)
    product = square(pair)
    for stage in range(ROUNDS // 2):
        early, late = 2 * stage, 2 * stage + 1
        arrived = exchange_all(product)
        product = product_halves(pair, prev)
        if late + 1 < ROUNDS:
            before = to_next(prev)
        both = pl.pallas_call(
            functools.partial(share_kernel, peers),
            out_shape=shape(PACKED + 4 * BW),
            compiler_params=PARAMS,
        )(arrived, product)
        both = exchange_all(both)
        gram, copies = pl.pallas_call(
            functools.partial(split_kernel, peers),
            out_shape=[shape(PACKED), shape(4 * BW)],
            compiler_params=PARAMS,
        )(both)
        cross_gram = exchange_all(copies)
        first = mover[early, 0] == 0
        a_moves = first != swapped
        move, stay = columns((gram,), labels_a, labels_b, swapped, a_moves)
        labels_a = stay[2 * BW + 1 : 2 * BW + 2]
        swapped = first
        sent = to_next(move)
        labels_b = sent[2 * BW + 1 : 2 * BW + 2]
        pair = rotate(pair, prev, stay, sent)
        if late + 1 < ROUNDS:
            prev_stay = to_next(stay)
            sent_before = to_next(sent)
            prev = join(prev, prev_stay, before, sent_before)
        if late + 1 == ROUNDS:
            a_moves = jnp.logical_not(swapped)
        else:
            first = mover[late, 0] == 0
            a_moves = first != swapped
        move, stay = columns((cross_gram, stay, sent), labels_a, labels_b, swapped, a_moves)
        if late + 1 == ROUNDS:
            return last(pair, move, stay)
        labels_a = stay[2 * BW + 1 : 2 * BW + 2]
        swapped = first
        sent = to_next(move)
        labels_b = sent[2 * BW + 1 : 2 * BW + 2]
        prev_stay = to_next(stay)
        pair, came, product = rotate(pair, prev, stay, sent, True)
        passed = to_next(came)
        prev = join(prev, prev_stay, passed)


def solution(mesh):
    placed = (P("rows", "blk"), P("blk"), P(None, "blk"))
    return jax.shard_map(
        body, mesh=mesh, in_specs=placed, out_specs=P("rows", "blk"), check_vma=False
    )
```

```python
import functools

import jax
import jax.numpy as jnp
from jax import lax
from jax.experimental import pallas as pl
from jax.experimental.pallas import tpu as pltpu
from jax.sharding import PartitionSpec as P

BW = 128
ROUNDS = 4
NS_STEPS = 3
ROW_TILE = 1024
PACKED = 5 * 64
PADDED = 8 * 64
PARAMS = pltpu.CompilerParams(vmem_limit_bytes=16 * 2**20)

epsilon = 1e-06
relaxation = 1.2
EXACT = lax.Precision.HIGHEST
F32 = jnp.float32


def mm(a, b):
    return jnp.dot(a, b, precision=EXACT, preferred_element_type=F32)


def mm_t(a, b):
    dims = (((0,), (0,)), ((), ()))
    return lax.dot_general(a, b, dims, precision=EXACT, preferred_element_type=F32)


def in_two(value):
    high = value.astype(jnp.bfloat16)
    return high, (value - high.astype(F32)).astype(jnp.bfloat16)


def apply(left, right):
    left_high, left_low = in_two(left)
    right_high, right_low = in_two(right)
    dot = functools.partial(jnp.dot, preferred_element_type=F32)
    return dot(left_high, right_high) + (dot(left_high, right_low) + dot(left_low, right_high))


def transposed_dot(left, right):
    dims = (((0,), (0,)), ((), ()))
    return lax.dot_general(left, right, dims, preferred_element_type=F32)


def unit():
    row = lax.broadcasted_iota(jnp.int32, (BW, BW), 0)
    return row, lax.broadcasted_iota(jnp.int32, (BW, BW), 1)


def product_kernel(left_ref, right_ref, out_ref):
    left_high, left_low = in_two(left_ref[...])
    right_high, right_low = in_two(right_ref[...])
    cross = transposed_dot(left_high, right_low) + transposed_dot(left_low, right_high)
    value = transposed_dot(left_high, right_high) + cross

    @pl.when(pl.program_id(0) == 0)
    def _():
        out_ref[...] = jnp.zeros_like(out_ref)

    out_ref[: 2 * BW, :] += value[:, :BW]
    out_ref[2 * BW :, :] += value[:, BW:]


def add_square(value, total_ref, out_ref):
    high, low = in_two(value)
    side = transposed_dot(high, low)
    value = transposed_dot(high, high) + (side + side.T)
    step = pl.program_id(0)

    @pl.when(step == 0)
    def _():
        total_ref[...] = value

    @pl.when(step > 0)
    def _():
        total_ref[...] += value

    @pl.when(step == pl.num_programs(0) - 1)
    def _():
        row, col = unit()
        second = total_ref[BW:, BW:]
        corner = total_ref[:BW, BW:]
        mixed = jnp.where(row <= col, total_ref[:BW, :BW], second)
        ends = jnp.sum(jnp.where(row == col, second, 0.0), axis=0, keepdims=True)
        ends = jnp.broadcast_to(ends, (PACKED - 2 * BW, BW))
        total_ref[:BW, :BW] = corner
        total_ref[BW:, :BW] = mixed
        for i in range(PADDED // 8):
            low = 5 * i
            inner = min(max(2 * BW - low, 0), 5)
            if inner:
                out_ref[8 * i : 8 * i + inner, :] = total_ref[low : low + inner, :BW]
            out_ref[8 * i + inner : 8 * (i + 1), :] = ends[: 8 - inner, :]


def unpacked(packed):
    row, col = unit()
    mixed = packed[BW : 2 * BW]
    turned = mixed.T
    ends = packed[2 * BW : 2 * BW + 1]
    first = jnp.where(row <= col, mixed, turned)
    second = jnp.where(row > col, mixed, jnp.where(row < col, turned, ends))
    return packed[:BW], first, second


def square_kernel(value_ref, out_ref, total_ref):
    add_square(value_ref[...], total_ref, out_ref)


TOTAL = pltpu.VMEM((2 * BW, 2 * BW), F32)


def tiled(width=2 * BW):
    return pl.BlockSpec((ROW_TILE, width), lambda i: (i, 0))


def whole(rows):
    return pl.BlockSpec((rows, BW), lambda i: (0, 0))


def shape(rows, cols=BW):
    return jax.ShapeDtypeStruct((rows, cols), F32)


def streamed(value):
    return pltpu.with_memory_space_constraint(value, pltpu.HBM)


def square(value):
    return pl.pallas_call(
        square_kernel,
        grid=(value.shape[0] // ROW_TILE,),
        in_specs=[tiled()],
        out_specs=whole(PADDED),
        out_shape=shape(PADDED),
        scratch_shapes=[TOTAL],
        compiler_params=PARAMS,
    )(streamed(value))


def product_halves(left, right):
    return pl.pallas_call(
        product_kernel,
        grid=(left.shape[0] // ROW_TILE,),
        in_specs=[tiled(), tiled()],
        out_specs=whole(4 * BW),
        out_shape=shape(4 * BW),
        compiler_params=PARAMS,
    )(streamed(left), right)


def share_kernel(peers, arrived_ref, lines_ref, out_ref):
    packed, lines = PACKED // peers, 4 * BW // peers
    padded = PADDED // peers
    part = arrived_ref[:padded, :]
    for i in range(1, peers):
        part += arrived_ref[padded * i : padded * (i + 1), :]
    part = jnp.concatenate([part[8 * k : 8 * k + 5] for k in range(padded // 8)], 0)
    for i in range(peers):
        at = (packed + lines) * i
        out_ref[at : at + packed, :] = part
        out_ref[at + packed : at + packed + lines, :] = lines_ref[lines * i : lines * (i + 1), :]


def split_kernel(peers, both_ref, packed_ref, out_ref):
    packed, lines = PACKED // peers, 4 * BW // peers
    part = both_ref[packed : packed + lines, :]
    for i in range(1, peers):
        at = (packed + lines) * i + packed
        part += both_ref[at : at + lines, :]
    for i in range(peers):
        out_ref[lines * i : lines * (i + 1), :] = part
    for i in range(peers):
        at = (packed + lines) * i
        packed_ref[packed * i : packed * (i + 1), :] = both_ref[at : at + packed, :]


def rotate_kernel(pair_ref, prev_ref, stay_ref, sent_ref, out_ref, came_ref=None, gram_ref=None, total_ref=None):
    came = apply(prev_ref[...], sent_ref[: 2 * BW, :])
    stays = apply(pair_ref[...], stay_ref[: 2 * BW, :])
    out_ref[:, :BW] = stays
    out_ref[:, BW:] = came
    if gram_ref is not None:
        came_ref[...] = came
        add_square(jnp.concatenate([stays, came], 1), total_ref, gram_ref)


def rotate(pair, prev, stay, sent, with_gram=False):
    rows = pair.shape[0]
    if with_gram:
        prev = streamed(prev)
    else:
        pair = streamed(pair)
    out_specs = (tiled(), tiled(BW), whole(PADDED))
    out_shape = (pltpu.HBM((rows, 2 * BW), F32), shape(rows), shape(PADDED))
    return pl.pallas_call(
        rotate_kernel,
        grid=(rows // ROW_TILE,),
        in_specs=[tiled(), tiled(), whole(stay.shape[0]), whole(sent.shape[0])],
        out_specs=out_specs if with_gram else out_specs[0],
        out_shape=out_shape if with_gram else out_shape[0],
        scratch_shapes=[TOTAL] if with_gram else [],
        compiler_params=PARAMS,
    )(pair, prev, stay, sent)


def join_kernel(prev_ref, cols_ref, passed_ref, out_ref):
    out_ref[:, :BW] = apply(prev_ref[...], cols_ref[: 2 * BW, :])
    out_ref[:, BW:] = passed_ref[...]


def join_two_kernel(prev_ref, cols_ref, other_ref, other_cols_ref, out_ref):
    out_ref[:, :BW] = apply(prev_ref[...], cols_ref[: 2 * BW, :])
    out_ref[:, BW:] = apply(other_ref[...], other_cols_ref[: 2 * BW, :])


def join(prev, cols, passed, passed_cols=None):
    rows = prev.shape[0]
    if passed_cols is None:
        prev, passed = streamed(prev), streamed(passed)
    args = (prev, cols, passed) if passed_cols is None else (prev, cols, passed, passed_cols)
    return pl.pallas_call(
        join_kernel if passed_cols is None else join_two_kernel,
        grid=(rows // ROW_TILE,),
        in_specs=[tiled(a.shape[1]) if a.shape[0] == rows else whole(a.shape[0]) for a in args],
        out_specs=tiled(),
        out_shape=shape(rows, 2 * BW) if passed_cols is None else pltpu.HBM((rows, 2 * BW), F32),
        compiler_params=PARAMS,
    )(*args)


def last_kernel(pair_ref, left_ref, right_ref, out_ref):
    pair = pair_ref[...]
    cols = jnp.concatenate([left_ref[: 2 * BW, :], right_ref[: 2 * BW, :]], 1)
    out_ref[...] = apply(pair, cols)


def last(pair, left, right):
    rows = pair.shape[0]
    return pl.pallas_call(
        last_kernel,
        grid=(rows // ROW_TILE,),
        in_specs=[tiled(), whole(left.shape[0]), whole(right.shape[0])],
        out_specs=tiled(),
        out_shape=shape(rows, 2 * BW),
        compiler_params=PARAMS,
    )(pair, left, right)


def form(halves, cols):
    return mm(halves[: 2 * BW], cols[:BW]) + mm(halves[2 * BW :], cols[BW:])


def columns_kernel(late, *refs):
    row_of, col_of = unit()
    keep = row_of == col_of
    eye = jnp.where(keep, 1.0, 0.0).astype(F32)

    def upright(row):
        return jnp.sum(jnp.where(keep, row, 0.0), axis=1, keepdims=True)

    if late:
        gram_ref, stay_ref, sent_ref, rows_ref, move_out, stay_out = refs
        gram = gram_ref[...]
        cross = mm_t(stay_ref[: 2 * BW, :], form(gram, sent_ref[: 2 * BW, :]))
        squares_a = stay_ref[2 * BW : 2 * BW + 1, :]
        squares_b = sent_ref[2 * BW : 2 * BW + 1, :]
    else:
        gram_ref, rows_ref, move_out, stay_out = refs
        cross, within_a, within_b = unpacked(gram_ref[...])
        squares_a = jnp.sum(jnp.where(keep, within_a, 0.0), axis=0, keepdims=True)
        squares_b = gram_ref[2 * BW : 2 * BW + 1, :]
        cross_t = cross.T
    labels_a, labels_b = rows_ref[0:1, :], rows_ref[1:2, :]
    sign, a_moves = rows_ref[2:3, :], rows_ref[3:4, :] > 0.5
    scale_a = upright(lax.rsqrt(squares_a + epsilon))
    scale_b = lax.rsqrt(squares_b + epsilon)
    gap = jnp.abs(upright(labels_a) - labels_b)
    scaled = cross * scale_a * scale_b / (1.0 + gap)
    total = jnp.sum(jnp.sum(scaled * scaled, axis=0, keepdims=True), axis=1, keepdims=True)
    gen = relaxation * scaled / jnp.sqrt(total + epsilon) * sign
    gen_t = gen.T
    factors = []
    corner = gen
    metrics = [eye + mm(gen, gen_t), eye + mm(gen_t, gen)]
    for sweep in range(NS_STEPS):
        steps = [1.5 * eye - 0.5 * metric for metric in metrics]
        factors = [mm(f, s) for f, s in zip(factors, steps)] if factors else steps
        corner = mm(corner, steps[1])
        if sweep + 1 < NS_STEPS:
            metrics = [mm(mm(m, s), s) for m, s in zip(metrics, steps)]
    corner_t = -corner.T
    row = lax.broadcasted_iota(jnp.int32, (8, BW), 0)
    for out_ref, pick in ((move_out, a_moves), (stay_out, jnp.logical_not(a_moves))):
        top = jnp.where(pick, factors[0], corner)
        bottom = jnp.where(pick, corner_t, factors[1])
        out_ref[:BW, :] = top
        out_ref[BW : 2 * BW, :] = bottom
        tail = jnp.where(row == 1, jnp.where(pick, labels_a, labels_b), 0.0)
        if not late:
            image_a = mm(within_a, top) + mm(cross, bottom)
            image_b = mm(cross_t, top) + mm(within_b, bottom)
            squares = jnp.sum(top * image_a + bottom * image_b, axis=0, keepdims=True)
            tail = jnp.where(row == 0, jnp.maximum(squares, 0.0), tail)
        out_ref[2 * BW :, :] = tail


def columns(args, labels_a, labels_b, swapped, a_moves):
    sign = jnp.where(swapped, -1.0, 1.0)
    pick = jnp.where(a_moves, 1.0, 0.0)
    row = lax.broadcasted_iota(jnp.int32, (8, BW), 0)
    rows = jnp.where(row == 2, sign, pick)
    rows = jnp.where(row == 0, labels_a, jnp.where(row == 1, labels_b, rows))
    return pl.pallas_call(
        functools.partial(columns_kernel, len(args) > 1),
        out_shape=[shape(2 * BW + 8)] * 2,
        compiler_params=PARAMS,
    )(*args, rows)


def exchange_all(parts):
    flat = parts.reshape(lax.axis_size("rows"), 1, -1)
    return lax.all_to_all(flat, "rows", split_axis=0, concat_axis=0, tiled=True).reshape(parts.shape)


def to_next(value):
    peers = lax.axis_size("blk")
    return lax.ppermute(value, "blk", [(i, (i + 1) % peers) for i in range(peers)])


def body(snapshots, grades, mover):
    peers = lax.axis_size("rows")
    labels = grades.astype(F32)
    labels_a, labels_b = labels[None, :BW], labels[None, BW:]
    swapped = jnp.zeros((), bool)
    pair = snapshots
    prev = to_next(pair)
    product = square(pair)
    for stage in range(ROUNDS // 2):
        early, late = 2 * stage, 2 * stage + 1
        arrived = exchange_all(product)
        product = product_halves(pair, prev)
        if late + 1 < ROUNDS:
            before = to_next(prev)
        both = pl.pallas_call(
            functools.partial(share_kernel, peers),
            out_shape=shape(PACKED + 4 * BW),
            compiler_params=PARAMS,
        )(arrived, product)
        both = exchange_all(both)
        gram, copies = pl.pallas_call(
            functools.partial(split_kernel, peers),
            out_shape=[shape(PACKED), shape(4 * BW)],
            compiler_params=PARAMS,
        )(both)
        cross_gram = exchange_all(copies)
        first = mover[early, 0] == 0
        a_moves = first != swapped
        move, stay = columns((gram,), labels_a, labels_b, swapped, a_moves)
        labels_a = stay[2 * BW + 1 : 2 * BW + 2]
        swapped = first
        sent = to_next(move)
        labels_b = sent[2 * BW + 1 : 2 * BW + 2]
        pair = rotate(pair, prev, stay, sent)
        if late + 1 < ROUNDS:
            prev_stay = to_next(stay)
            sent_before = to_next(sent)
            prev = join(prev, prev_stay, before, sent_before)
        if late + 1 == ROUNDS:
            a_moves = jnp.logical_not(swapped)
        else:
            first = mover[late, 0] == 0
            a_moves = first != swapped
        move, stay = columns((cross_gram, stay, sent), labels_a, labels_b, swapped, a_moves)
        if late + 1 == ROUNDS:
            return last(pair, move, stay)
        labels_a = stay[2 * BW + 1 : 2 * BW + 2]
        swapped = first
        sent = to_next(move)
        labels_b = sent[2 * BW + 1 : 2 * BW + 2]
        prev_stay = to_next(stay)
        pair, came, product = rotate(pair, prev, stay, sent, True)
        passed = to_next(came)
        prev = join(prev, prev_stay, passed)


def solution(mesh):
    placed = (P("rows", "blk"), P("blk"), P(None, "blk"))
    return jax.shard_map(
        body, mesh=mesh, in_specs=placed, out_specs=P("rows", "blk"), check_vma=False
    )
```

```python
import functools

import jax
import jax.numpy as jnp
from jax import lax
from jax.experimental import pallas as pl
from jax.experimental.pallas import tpu as pltpu
from jax.sharding import PartitionSpec as P

BW = 128
ROUNDS = 4
NS_STEPS = 3
ROW_TILE = 1024
PACKED = 5 * 64
PADDED = 8 * 64
PARAMS = pltpu.CompilerParams(vmem_limit_bytes=16 * 2**20)

epsilon = 1e-06
relaxation = 1.2
EXACT = lax.Precision.HIGHEST
F32 = jnp.float32


def mm(a, b):
    return jnp.dot(a, b, precision=EXACT, preferred_element_type=F32)


def mm_t(a, b):
    dims = (((0,), (0,)), ((), ()))
    return lax.dot_general(a, b, dims, precision=EXACT, preferred_element_type=F32)


def in_two(value):
    high = value.astype(jnp.bfloat16)
    return high, (value - high.astype(F32)).astype(jnp.bfloat16)


def apply(left, right):
    left_high, left_low = in_two(left)
    right_high, right_low = in_two(right)
    dot = functools.partial(jnp.dot, preferred_element_type=F32)
    return dot(left_high, right_high) + (dot(left_high, right_low) + dot(left_low, right_high))


def transposed_dot(left, right):
    dims = (((0,), (0,)), ((), ()))
    return lax.dot_general(left, right, dims, preferred_element_type=F32)


def unit():
    row = lax.broadcasted_iota(jnp.int32, (BW, BW), 0)
    return row, lax.broadcasted_iota(jnp.int32, (BW, BW), 1)


def add_product(left, right, *out_refs):
    left_high, left_low = in_two(left)
    right_high, right_low = in_two(right)
    cross = transposed_dot(left_high, right_low) + transposed_dot(left_low, right_high)
    value = transposed_dot(left_high, right_high) + cross
    for k, out_ref in enumerate(out_refs):
        block = value[:, BW * k : BW * (k + 1)]

        @pl.when(pl.program_id(0) == 0)
        def _(out_ref=out_ref, block=block):
            out_ref[...] = block

        @pl.when(pl.program_id(0) > 0)
        def _(out_ref=out_ref, block=block):
            out_ref[...] += block


def product_kernel(left_ref, right_ref, *out_refs):
    add_product(left_ref[...], right_ref[...], *out_refs)


def stay_product_kernel(left_ref, prev_ref, cols_ref, out_ref, product_ref):
    value = apply(prev_ref[...], cols_ref[: 2 * BW, :])
    out_ref[...] = value
    add_product(left_ref[...], value, product_ref)


def add_square(value, total_ref, out_ref):
    high, low = in_two(value)
    side = transposed_dot(high, low)
    value = transposed_dot(high, high) + (side + side.T)
    step = pl.program_id(0)

    @pl.when(step == 0)
    def _():
        total_ref[...] = value

    @pl.when(step > 0)
    def _():
        total_ref[...] += value

    @pl.when(step == pl.num_programs(0) - 1)
    def _():
        row, col = unit()
        second = total_ref[BW:, BW:]
        corner = total_ref[:BW, BW:]
        mixed = jnp.where(row <= col, total_ref[:BW, :BW], second)
        ends = jnp.sum(jnp.where(row == col, second, 0.0), axis=0, keepdims=True)
        ends = jnp.broadcast_to(ends, (PACKED - 2 * BW, BW))
        total_ref[:BW, :BW] = corner
        total_ref[BW:, :BW] = mixed
        for i in range(PADDED // 8):
            low = 5 * i
            inner = min(max(2 * BW - low, 0), 5)
            if inner:
                out_ref[8 * i : 8 * i + inner, :] = total_ref[low : low + inner, :BW]
            out_ref[8 * i + inner : 8 * (i + 1), :] = ends[: 8 - inner, :]


def unpacked(packed):
    row, col = unit()
    mixed = packed[BW : 2 * BW]
    turned = mixed.T
    ends = packed[2 * BW : 2 * BW + 1]
    first = jnp.where(row <= col, mixed, turned)
    second = jnp.where(row > col, mixed, jnp.where(row < col, turned, ends))
    return packed[:BW], first, second


def square_kernel(value_ref, out_ref, total_ref):
    add_square(value_ref[...], total_ref, out_ref)


TOTAL = pltpu.VMEM((2 * BW, 2 * BW), F32)


def tiled(width=2 * BW):
    return pl.BlockSpec((ROW_TILE, width), lambda i: (i, 0))


def whole(rows):
    return pl.BlockSpec((rows, BW), lambda i: (0, 0))


def shape(rows, cols=BW):
    return jax.ShapeDtypeStruct((rows, cols), F32)


def streamed(value):
    return pltpu.with_memory_space_constraint(value, pltpu.HBM)


def square(value):
    return pl.pallas_call(
        square_kernel,
        grid=(value.shape[0] // ROW_TILE,),
        in_specs=[tiled()],
        out_specs=whole(PADDED),
        out_shape=shape(PADDED),
        scratch_shapes=[TOTAL],
        compiler_params=PARAMS,
    )(streamed(value))


def product(left, right):
    blocks = right.shape[1] // BW
    return pl.pallas_call(
        product_kernel,
        grid=(left.shape[0] // ROW_TILE,),
        in_specs=[tiled(), tiled(right.shape[1])],
        out_specs=[whole(2 * BW)] * blocks,
        out_shape=[shape(2 * BW)] * blocks,
        compiler_params=PARAMS,
    )(streamed(left), right)


def stay_product(left, prev, cols):
    rows = left.shape[0]
    return pl.pallas_call(
        stay_product_kernel,
        grid=(rows // ROW_TILE,),
        in_specs=[tiled(), tiled(), whole(cols.shape[0])],
        out_specs=[tiled(BW), whole(2 * BW)],
        out_shape=[shape(rows), shape(2 * BW)],
        compiler_params=PARAMS,
    )(streamed(left), streamed(prev), cols)


def share_kernel(peers, arrived_ref, first_ref, second_ref, out_ref):
    packed, lines = PACKED // peers, 4 * BW // peers
    padded = PADDED // peers
    part = arrived_ref[:padded, :]
    for i in range(1, peers):
        part += arrived_ref[padded * i : padded * (i + 1), :]
    part = jnp.concatenate([part[8 * k : 8 * k + 5] for k in range(padded // 8)], 0)
    for i in range(peers):
        at = (packed + lines) * i
        out_ref[at : at + packed, :] = part
        half = peers // 2
        lines_ref, line = (first_ref, lines * i) if i < half else (second_ref, lines * (i - half))
        out_ref[at + packed : at + packed + lines, :] = lines_ref[line : line + lines, :]


def split_kernel(peers, both_ref, packed_ref, out_ref):
    packed, lines = PACKED // peers, 4 * BW // peers
    part = both_ref[packed : packed + lines, :]
    for i in range(1, peers):
        at = (packed + lines) * i + packed
        part += both_ref[at : at + lines, :]
    for i in range(peers):
        out_ref[lines * i : lines * (i + 1), :] = part
    for i in range(peers):
        at = (packed + lines) * i
        packed_ref[packed * i : packed * (i + 1), :] = both_ref[at : at + packed, :]


def rotated(pair_ref, prev_refs, stay_ref, sent_ref, out_ref):
    width = 2 * BW // len(prev_refs)
    came = 0.0
    for k, prev_ref in enumerate(prev_refs):
        came += apply(prev_ref[...], sent_ref[width * k : width * (k + 1), :])
    stays = apply(pair_ref[...], stay_ref[: 2 * BW, :])
    out_ref[:, :BW] = stays
    out_ref[:, BW:] = came
    return stays, came


def rotate_kernel(pair_ref, *refs):
    *prev_refs, stay_ref, sent_ref, out_ref = refs
    rotated(pair_ref, prev_refs, stay_ref, sent_ref, out_ref)


def rotate_square_kernel(pair_ref, prev_ref, stay_ref, sent_ref, out_ref, came_ref, square_ref, total_ref):
    stays, came = rotated(pair_ref, [prev_ref], stay_ref, sent_ref, out_ref)
    came_ref[...] = came
    add_square(jnp.concatenate([stays, came], 1), total_ref, square_ref)


def rotate(pair, prev, stay, sent):
    rows = pair.shape[0]
    return pl.pallas_call(
        rotate_kernel,
        grid=(rows // ROW_TILE,),
        in_specs=[tiled(), *(tiled(p.shape[1]) for p in prev), whole(stay.shape[0]), whole(sent.shape[0])],
        out_specs=tiled(),
        out_shape=pltpu.HBM((rows, 2 * BW), F32),
        compiler_params=PARAMS,
    )(streamed(pair), *prev, stay, sent)


def rotate_square(pair, prev, stay, sent):
    rows = pair.shape[0]
    return pl.pallas_call(
        rotate_square_kernel,
        grid=(rows // ROW_TILE,),
        in_specs=[tiled(), tiled(), whole(stay.shape[0]), whole(sent.shape[0])],
        out_specs=[tiled(), tiled(BW), whole(PADDED)],
        out_shape=[pltpu.HBM((rows, 2 * BW), F32), shape(rows), shape(PADDED)],
        scratch_shapes=[TOTAL],
        compiler_params=PARAMS,
    )(pair, streamed(prev), stay, sent)


def join_kernel(prev_ref, cols_ref, other_ref, other_cols_ref, out_ref):
    out_ref[:, :BW] = apply(prev_ref[...], cols_ref[: 2 * BW, :])
    out_ref[:, BW:] = apply(other_ref[...], other_cols_ref[: 2 * BW, :])


def join(*args):
    rows = args[0].shape[0]
    return pl.pallas_call(
        join_kernel,
        grid=(rows // ROW_TILE,),
        in_specs=[tiled(a.shape[1]) if a.shape[0] == rows else whole(a.shape[0]) for a in args],
        out_specs=tiled(),
        out_shape=pltpu.HBM((rows, 2 * BW), F32),
        compiler_params=PARAMS,
    )(*args)


def last_kernel(pair_ref, left_ref, right_ref, out_ref):
    pair = pair_ref[...]
    cols = jnp.concatenate([left_ref[: 2 * BW, :], right_ref[: 2 * BW, :]], 1)
    out_ref[...] = apply(pair, cols)


def last(pair, left, right):
    pair = streamed(pair)
    rows = pair.shape[0]
    return pl.pallas_call(
        last_kernel,
        grid=(rows // ROW_TILE,),
        in_specs=[tiled(), whole(left.shape[0]), whole(right.shape[0])],
        out_specs=tiled(),
        out_shape=shape(rows, 2 * BW),
        compiler_params=PARAMS,
    )(pair, left, right)


def form(halves, cols):
    return mm(halves[: 2 * BW], cols[:BW]) + mm(halves[2 * BW :], cols[BW:])


def columns_kernel(late, *refs):
    row_of, col_of = unit()
    keep = row_of == col_of
    eye = jnp.where(keep, 1.0, 0.0).astype(F32)

    def upright(row):
        return jnp.sum(jnp.where(keep, row, 0.0), axis=1, keepdims=True)

    if late:
        gram_ref, stay_ref, sent_ref, rows_ref, move_out, stay_out = refs
        gram = gram_ref[...]
        cross = mm_t(stay_ref[: 2 * BW, :], form(gram, sent_ref[: 2 * BW, :]))
        squares_a = stay_ref[2 * BW : 2 * BW + 1, :]
        squares_b = sent_ref[2 * BW : 2 * BW + 1, :]
    else:
        gram_ref, rows_ref, move_out, stay_out = refs
        cross, within_a, within_b = unpacked(gram_ref[...])
        squares_a = jnp.sum(jnp.where(keep, within_a, 0.0), axis=0, keepdims=True)
        squares_b = gram_ref[2 * BW : 2 * BW + 1, :]
        cross_t = cross.T
    labels_a, labels_b = rows_ref[0:1, :], rows_ref[1:2, :]
    sign, a_moves = rows_ref[2:3, :], rows_ref[3:4, :] > 0.5
    scale_a = upright(lax.rsqrt(squares_a + epsilon))
    scale_b = lax.rsqrt(squares_b + epsilon)
    gap = jnp.abs(upright(labels_a) - labels_b)
    scaled = cross * scale_a * scale_b / (1.0 + gap)
    total = jnp.sum(jnp.sum(scaled * scaled, axis=0, keepdims=True), axis=1, keepdims=True)
    gen = relaxation * scaled / jnp.sqrt(total + epsilon) * sign
    gen_t = gen.T
    factors = []
    corner = gen
    metrics = [eye + mm(gen, gen_t), eye + mm(gen_t, gen)]
    for sweep in range(NS_STEPS):
        steps = [1.5 * eye - 0.5 * metric for metric in metrics]
        factors = [mm(f, s) for f, s in zip(factors, steps)] if factors else steps
        corner = mm(corner, steps[1])
        if sweep + 1 < NS_STEPS:
            metrics = [mm(mm(m, s), s) for m, s in zip(metrics, steps)]
    corner_t = -corner.T
    row = lax.broadcasted_iota(jnp.int32, (8, BW), 0)
    for out_ref, pick in ((move_out, a_moves), (stay_out, jnp.logical_not(a_moves))):
        top = jnp.where(pick, factors[0], corner)
        bottom = jnp.where(pick, corner_t, factors[1])
        out_ref[:BW, :] = top
        out_ref[BW : 2 * BW, :] = bottom
        tail = jnp.where(row == 1, jnp.where(pick, labels_a, labels_b), 0.0)
        if not late:
            image_a = mm(within_a, top) + mm(cross, bottom)
            image_b = mm(cross_t, top) + mm(within_b, bottom)
            squares = jnp.sum(top * image_a + bottom * image_b, axis=0, keepdims=True)
            tail = jnp.where(row == 0, jnp.maximum(squares, 0.0), tail)
        out_ref[2 * BW :, :] = tail


def columns(args, labels_a, labels_b, swapped, a_moves):
    sign = jnp.where(swapped, -1.0, 1.0)
    pick = jnp.where(a_moves, 1.0, 0.0)
    row = lax.broadcasted_iota(jnp.int32, (8, BW), 0)
    rows = jnp.where(row == 2, sign, pick)
    rows = jnp.where(row == 0, labels_a, jnp.where(row == 1, labels_b, rows))
    return pl.pallas_call(
        functools.partial(columns_kernel, len(args) > 1),
        out_shape=[shape(2 * BW + 8)] * 2,
        compiler_params=PARAMS,
    )(*args, rows)


def exchange_all(parts):
    flat = parts.reshape(lax.axis_size("rows"), 1, -1)
    return lax.all_to_all(flat, "rows", split_axis=0, concat_axis=0, tiled=True).reshape(parts.shape)


def to_next(value):
    peers = lax.axis_size("blk")
    return lax.ppermute(value, "blk", [(i, (i + 1) % peers) for i in range(peers)])


def body(snapshots, grades, mover):
    peers = lax.axis_size("rows")
    labels = grades.astype(F32)
    labels_a, labels_b = labels[None, :BW], labels[None, BW:]
    swapped = jnp.zeros((), bool)
    pair = snapshots
    prev = to_next(pair)
    squares = square(pair)
    for stage in range(ROUNDS // 2):
        early, late = 2 * stage, 2 * stage + 1
        arrived = exchange_all(squares)
        if stage == 0:
            lines = product(pair, prev)
            prev_parts = [prev]
        else:
            kept, lines = stay_product(pair, prev, prev_stay)
            lines = [lines, *product(pair, passed)]
            prev_parts = [kept, passed]
        if late + 1 < ROUNDS:
            before = to_next(prev)
        both = pl.pallas_call(
            functools.partial(share_kernel, peers),
            out_shape=shape(PACKED + 4 * BW),
            compiler_params=PARAMS,
        )(arrived, *lines)
        both = exchange_all(both)
        gram, copies = pl.pallas_call(
            functools.partial(split_kernel, peers),
            out_shape=[shape(PACKED), shape(4 * BW)],
            compiler_params=PARAMS,
        )(both)
        cross_gram = exchange_all(copies)
        first = mover[early, 0] == 0
        a_moves = first != swapped
        move, stay = columns((gram,), labels_a, labels_b, swapped, a_moves)
        labels_a = stay[2 * BW + 1 : 2 * BW + 2]
        swapped = first
        sent = to_next(move)
        labels_b = sent[2 * BW + 1 : 2 * BW + 2]
        pair = rotate(pair, prev_parts, stay, sent)
        if late + 1 < ROUNDS:
            prev_stay = to_next(stay)
            sent_before = to_next(sent)
            prev = join(prev, prev_stay, before, sent_before)
        if late + 1 == ROUNDS:
            a_moves = jnp.logical_not(swapped)
        else:
            first = mover[late, 0] == 0
            a_moves = first != swapped
        move, stay = columns((cross_gram, stay, sent), labels_a, labels_b, swapped, a_moves)
        if late + 1 == ROUNDS:
            return last(pair, move, stay)
        labels_a = stay[2 * BW + 1 : 2 * BW + 2]
        swapped = first
        sent = to_next(move)
        labels_b = sent[2 * BW + 1 : 2 * BW + 2]
        prev_stay = to_next(stay)
        pair, came, squares = rotate_square(pair, prev, stay, sent)
        passed = to_next(came)


def solution(mesh):
    placed = (P("rows", "blk"), P("blk"), P(None, "blk"))
    return jax.shard_map(
        body, mesh=mesh, in_specs=placed, out_specs=P("rows", "blk"), check_vma=False
    )
```
